32 devices in a mesh: leaf: 16 (over z, y, x), sep: 2 (over core).
Axes of the slice: x: 2, y: 2, z: 4, core: 2. Of those that a mesh axis runs over, the one named last changes fastest.
Arguments:
- leaf_rhs: bfloat16 [16, 256, 2048], P('leaf', None, 'sep'), may hold values from -6 to 6
- leaf_inv: bfloat16 [16, 2048, 2048], P('leaf', 'sep'), may hold values from -0.125 to 0.125
- leaf_couple: bfloat16 [16, 512, 2048], P('leaf', None, 'sep'), may hold values from -0.0625 to 0.0625
- sep_rhs: float32 [16, 256, 512], P('leaf', None, 'sep'), may hold values from -6 to 6
- sep_inv: float32 [16, 512, 512], P('leaf', 'sep'), may hold values from -0.25 to 0.25
- sep_couple: float32 [16, 512, 512], P('leaf', None, 'sep'), may hold values from -0.1875 to 0.1875
Outputs:
- leaf_solution: float32 [16, 256, 2048], P('leaf', None, 'sep')
- sep_solution: float32 [16, 256, 512], P('leaf', None, 'sep')
The draws below stay inside these ranges and needn't reach their ends.
All inputs are finite; a program needn't handle non-finite values.
Results may differ from the reference program's by a relative error of at most 0.0042.
Values may be sent and summed in bfloat16 or wider, within the bound.
A program may use at most 128 MiB of HBM per device.

```python
import jax
import jax.numpy as jnp
import numpy as np
from jax import lax

NI = 2048
S = 512
RHS = 256
LEAVES = 16
LEVELS = 4


def levels(key, extent, shards, smallest, high):
    factor_of = 1.0
    for axis_at, parts in shards:
        steps = jax.random.uniform(jax.random.fold_in(jax.random.fold_in(key, 6), axis_at), (parts,), jnp.float32, smallest / len(shards), high / len(shards))
        factor_of = factor_of * jnp.repeat(jnp.exp(steps), extent[axis_at] // parts).reshape((-1,) + (1,) * (len(extent) - 1 - axis_at))
    return factor_of


def gaussian(key, shape, deviation, most, shards=(), held_as=jnp.bfloat16):
    result = jax.random.normal(key, shape, jnp.float32) * deviation
    if len(shards) > 0:
        result = levels(key, shape, shards, -0.22, 0.18) * result
    return jnp.clip(result, min=-most, max=most).astype(held_as)


def setup_inputs(seed: int = 0) -> dict:
    arg_keys = jax.random.split(jax.random.key(seed), 7)
    return {
        "leaf_rhs": gaussian(arg_keys[0], (LEAVES, RHS, NI), 1.0, 6.0, ((0, 16), (2, 2))),
        "leaf_inv": gaussian(arg_keys[1], (LEAVES, NI, NI), NI ** -0.5, 0.125, ((0, 16), (1, 2))),
        "leaf_couple": gaussian(arg_keys[2], (LEAVES, S, NI), (4 * NI) ** -0.5, 0.0625, ((0, 16), (2, 2))),
        "sep_rhs": gaussian(arg_keys[3], (LEAVES, RHS, S), 1.0, 6.0, ((0, 16), (2, 2)), jnp.float32),
        "sep_inv": gaussian(arg_keys[4], (LEAVES, S, S), S ** -0.5, 0.25, ((0, 16), (1, 2)), jnp.float32),
        "sep_couple": gaussian(arg_keys[5], (LEAVES, S, S), (2 * S) ** -0.5, 0.1875, ((0, 16), (2, 2)), jnp.float32),
    }


def leaf_up(items):
    rhs, inverse, couple = items
    dims = (((1,), (1,)), ((), ()))
    state = lax.dot_general(rhs, inverse, dims, preferred_element_type=jnp.float32).astype(jnp.bfloat16)
    return state, lax.dot_general(state, couple, dims, preferred_element_type=jnp.float32)


def leaf_down(items):
    state, parent, couple, inverse = items
    pulled = jnp.dot(parent.astype(jnp.bfloat16), couple, preferred_element_type=jnp.float32)
    residue = (state.astype(jnp.float32) - pulled).astype(jnp.bfloat16)
    return jnp.dot(residue, inverse, preferred_element_type=jnp.float32)


def reference(leaf_rhs, leaf_inv, leaf_couple, sep_rhs, sep_inv, sep_couple):
    count = leaf_rhs.shape[0]
    high = lax.Precision.HIGHEST
    leaf_state, leaf_out = lax.map(leaf_up, (leaf_rhs, leaf_inv, leaf_couple))
    sep_state = jnp.zeros(sep_rhs.shape, jnp.float32)
    outgoing = leaf_out
    for section in range(1, LEVELS + 2):
        slots = np.arange(2 ** (section - 1) - 1, count, 2 ** section)
        if section == 1:
            children = outgoing[slots] + outgoing[slots + 1]
        elif section <= LEVELS:
            reach = 2 ** (section - 2)
            children = outgoing[slots - reach] + outgoing[slots + reach]
        else:
            children = outgoing[slots - 2 ** (section - 2)]
        work = sep_rhs[slots] - children
        fresh = jnp.einsum("brk,bmk->brm", work, sep_inv[slots], precision=high)
        sep_state = sep_state.at[slots].set(fresh)
        if section <= LEVELS:
            sent = jnp.einsum("brk,bmk->brm", fresh, sep_couple[slots], precision=high)
            outgoing = jnp.zeros(sep_rhs.shape, jnp.float32).at[slots].set(sent)
    sep_solution = jnp.zeros(sep_rhs.shape, jnp.float32)
    for section in range(LEVELS + 1, 0, -1):
        slots = np.arange(2 ** (section - 1) - 1, count, 2 ** section)
        if section == LEVELS + 1:
            work = sep_state[slots]
        else:
            reach = 2 ** (section - 1)
            parent = np.where(((slots >> section) & 1) == 0, slots + reach, slots - reach)
            work = sep_state[slots] - jnp.einsum("brk,bkm->brm", sep_solution[parent], sep_couple[slots], precision=high)
        solved = jnp.einsum("brk,bkm->brm", work, sep_inv[slots], precision=high)
        sep_solution = sep_solution.at[slots].set(solved)
    numbers = np.arange(count)
    parents = numbers - numbers % 2
    leaf_solution = lax.map(leaf_down, (leaf_state, sep_solution[parents], leaf_couple, leaf_inv))
    return leaf_solution, sep_solution
```

```python
import functools

import jax
import jax.numpy as jnp
from jax import lax
from jax.experimental import pallas as pl
from jax.experimental.pallas import tpu as pltpu
from jax.sharding import PartitionSpec as P

F32 = jnp.float32
BF16 = jnp.bfloat16


def dot_nt(a, b):
    return lax.dot_general(a, b, (((1,), (1,)), ((), ())), preferred_element_type=F32)


def dot_nn(a, b):
    return lax.dot_general(a, b, (((1,), (0,)), ((), ())), preferred_element_type=F32)


def dot_tn(a, b):
    return lax.dot_general(a, b, (((0,), (0,)), ((), ())), preferred_element_type=F32)


def halves(value):
    high = value.astype(BF16)
    return high, (value - high.astype(F32)).astype(BF16)


def three_pass(a, b, dot):
    ah, al = halves(a)
    bh, bl = halves(b)
    return dot(ah, bh) + (dot(ah, bl) + dot(al, bh))


def two_pass(a, b, dot):
    rows = a.shape[0]
    both = dot(jnp.concatenate(halves(a), axis=0), b)
    return both[:rows] + both[rows:]


def kernel(
    leaves,
    rhs_ref, inv_hbm, couple_hbm, srhs_ref, sinv_ref, scpl_ref,
    leaf_out, sep_out,
    inv, couple, other_rhs, state, other_inv, other_cpl, fac, top,
    r1, rb, rt, part_send, part_own, part_recv, xs, xr, o1, yr,
    zs, zr, sols, dn, s2, s1, gath, fin_s, fin_r, sep_acc,
    load_sem, send_sem, recv_sem, rsend, rrecv, osend, orecv,
):
    p = lax.axis_index("leaf")
    c = lax.axis_index("sep")
    oc = 1 - c
    b0 = p % 2
    b1 = (p // 2) % 2
    q = p // 4
    planes = leaves // 4
    below_top = planes // 2 - 1
    xp = p + 1 - 2 * b0
    yp = p + 2 - 4 * b1
    rows = rhs_ref.shape[0]
    part = rhs_ref.shape[1]
    width = sinv_ref.shape[1]
    half = width // 2
    quarter = rows // 4
    eighth = rows // 8

    loads = [
        pltpu.make_async_copy(couple_hbm.at[0], couple, load_sem.at[0]),
        pltpu.make_async_copy(inv_hbm.at[0], inv, load_sem.at[1]),
    ]
    for copy in loads:
        copy.start()

    me = p * 2 + c
    count = 2 * leaves
    barrier = pltpu.get_barrier_semaphore()

    @pl.loop(1, count)
    def _(step):
        to = (me + step) % count
        pl.semaphore_signal(barrier, inc=1, device_id=(to // 2, to % 2), device_id_type=pl.DeviceIdType.MESH)

    pl.semaphore_wait(barrier, count - 1)

    pending = []

    def remote(src, dst, ssem, rsem, to):
        return pltpu.make_async_remote_copy(
            src_ref=src, dst_ref=dst, send_sem=ssem, recv_sem=rsem,
            device_id=to, device_id_type=pl.DeviceIdType.MESH,
        )

    def when(cond, action):
        if cond is None:
            action()
        else:
            @pl.when(cond)
            def _():
                action()

    def push(src, dst, ssem, rsem, to, cond=None):
        copy = remote(src, dst, ssem, rsem, to)
        when(cond, lambda: copy.start())
        pending.append((cond, copy))

    def arrive(dst, rsem, cond=None):
        copy = remote(dst, dst, send_sem.at[0], rsem, (p, oc))
        when(cond, lambda: copy.wait_recv())

    def send(src, dst, slot, to, cond=None):
        push(src, dst, send_sem.at[slot], recv_sem.at[slot], to, cond)

    def got(dst, slot, cond=None):
        arrive(dst, recv_sem.at[slot], cond)

    mate = (p, oc)
    send(sinv_ref, other_inv, 1, mate)
    send(scpl_ref.at[pl.ds(pl.multiple_of(oc * half, half), half)], other_cpl, 2, mate)
    send(rhs_ref, other_rhs, 0, mate)

    is_even = b0 == 0
    is_top = p == leaves - 1
    for t in range(4):
        tc, tb0 = t // 2, t % 2
        to = (p - b0 + tb0, tc)
        mine = (c == tc) & (b0 == tb0)
        push(
            srhs_ref.at[pl.ds(t * quarter, quarter)], r1.at[c], rsend.at[t], rrecv.at[c],
            to, is_even & jnp.logical_not(mine),
        )

        @pl.when(is_even & mine)
        def _():
            r1[c] = srhs_ref[pl.ds(t * quarter, quarter), :]

    is_odd = (b0 == 1) & jnp.logical_not(is_top)
    for t in range(8):
        tc, tb0, tb1 = t // 4, (t // 2) % 2, t % 2
        to = (4 * q + 2 * tb1 + tb0, tc)
        mine = (c == tc) & (b0 == tb0) & (b1 == tb1)
        block = srhs_ref.at[pl.ds(t * eighth, eighth)]
        push(block, rb.at[b1, c], rsend.at[4 + t], rrecv.at[2 + 2 * b1 + c], to, is_odd & jnp.logical_not(mine))

        @pl.when(is_odd & mine)
        def _():
            rb[b1, c] = srhs_ref[pl.ds(t * eighth, eighth), :]

        to = (4 * below_top + 2 * tb1 + tb0, tc)
        push(block, rt.at[c], rsend.at[12 + t], rrecv.at[6 + c], to, is_top)

    own = b0 * (1 + b1)
    got(other_inv, 1)
    got(other_cpl, 2)
    at = pl.ds(pl.multiple_of(c * half, half), half)
    ours = scpl_ref[at, :]
    m_rows = three_pass(ours, sinv_ref[...], dot_nn) + three_pass(other_cpl[...], other_inv[...], dot_nn)
    n_rows = three_pass(sinv_ref[:, at], sinv_ref[...], dot_tn) + three_pass(other_inv[:, at], other_inv[...], dot_tn)
    fac[0, own, c] = jnp.where(is_top, n_rows, m_rows).astype(BF16)
    fac[1, own, c] = n_rows.astype(BF16)
    theirs = (1 - b0) * (1 + b1)
    carried = 1 + b1
    across = 2 - b1

    def factor_x(kind):
        base = 3 + 5 * kind
        ref = fac.at[kind, own, c]
        send(ref, ref, base + 1, (xp, c))
        send(ref, ref, base, mate)

    def factor_y(kind):
        base = 3 + 5 * kind
        ref = fac.at[kind, theirs, c]
        got(ref, base + 1)
        ref2 = fac.at[kind, carried, c]
        send(ref2, ref2, base + 3, (yp, c))
        send(ref, ref, base + 2, mate)

    def factor_end(kind):
        base = 3 + 5 * kind
        ref = fac.at[kind, across, c]
        got(ref, base + 3)
        send(ref, ref, base + 4, mate)

    def factor_wait(kind, which):
        base = 3 + 5 * kind
        idx, slot = ((own, base), (theirs, base + 2), (across, base + 4))[which]
        got(fac.at[kind, idx, oc], slot)

    def factor(kind, idx):
        return fac[kind, idx].reshape(width, width)

    factor_x(0)

    got(other_rhs, 0)
    loads[1].wait()
    mine_cols = pl.ds(pl.multiple_of(c * part, part), part)
    other_cols = pl.ds(pl.multiple_of(oc * part, part), part)
    piece = part // 4
    for j in range(4):
        at_j = pl.ds(j * piece, piece)
        value = dot_nt(rhs_ref[...], inv[at_j, mine_cols]) + dot_nt(other_rhs[...], inv[at_j, other_cols])
        state[:, at_j] = value.astype(BF16)
    loads[0].wait()
    mid = rows // 2
    part_send[...] = dot_nt(
        state[pl.ds(pl.multiple_of(oc * mid, mid), mid), :], couple[...]
    ).reshape(2, quarter, width)
    send(part_send, part_recv, 13, mate)
    part_own[...] = dot_nt(
        state[pl.ds(pl.multiple_of(c * mid, mid), mid), :], couple[...]
    ).reshape(2, quarter, width)
    got(part_recv, 13)
    xs[...] = part_own[1 - b0] + part_recv[1 - b0]
    send(xs, xr, 14, (xp, c))
    factor_x(1)
    factor_y(0)
    factor_wait(0, 0)
    factor_wait(0, 1)

    for h in range(2):
        arrive(r1.at[h], rrecv.at[h], jnp.logical_not(is_even & (c == h)))
    got(xr, 14)
    taken = part_own[b0] + part_recv[b0] + xr[...]
    w1 = jnp.concatenate([r1[0], r1[1]], axis=1) - taken
    o1[...] = two_pass(w1, factor(0, 0), dot_nt).reshape(2, eighth, width)
    send(o1.at[1 - b1], yr, 15, (yp, c))
    factor_end(0)
    factor_wait(0, 2)
    last = q == planes - 1
    joint = q == below_top
    send(fac.at[0, 2, c], top.at[c], 16, (4 * below_top + p % 4, c), last)

    for h in range(2):
        arrive(rb.at[0, h], rrecv.at[2 + h], jnp.logical_not((b0 == 1) & (b1 == 0) & (c == h)))
    got(yr, 15)
    w2 = jnp.concatenate([rb[0, 0], rb[0, 1]], axis=1) - (o1[b1] + yr[...])
    out2 = two_pass(w2, factor(0, 1), dot_nt)
    even_plane = q % 2 == 0
    odd_plane = jnp.logical_not(even_plane)
    zs[0] = out2
    place = p % 4
    send(zs.at[0], zr.at[1], 19, (4 * (q - 1) + place, c), odd_plane)

    reach = 1
    for bit in range(leaves.bit_length()):
        reach = jnp.where((q + 1) % (2 ** (bit + 1)) == 0, 2 ** (bit + 1), reach)
    upper = (q // (2 * reach)) % 2 == 1
    parent = jnp.where(upper, q - reach, q + reach)
    has_node = jnp.logical_not(last)
    low_child = q - reach // 2
    high_child = q + reach // 2
    inner = odd_plane & has_node

    factor_y(1)
    got(top.at[c], 16, joint)
    send(top.at[c], top.at[c], 17, mate, joint)

    for h in range(2):
        arrive(rb.at[1, h], rrecv.at[4 + h], has_node & jnp.logical_not((b0 == 1) & (b1 == 1) & (c == h)))
    got(zr.at[0], 18, inner)
    got(zr.at[1], 19, has_node)
    w3_at = s2.at[0]

    @pl.when(has_node)
    def _():
        first = jnp.where(even_plane, zs[0], zr[0])
        w3 = jnp.concatenate([rb[1, 0], rb[1, 1]], axis=1) - (first + zr[1])
        w3_at[...] = w3
        zs[1] = two_pass(w3, factor(0, 2), dot_nt)

    climbs = has_node & jnp.logical_not(joint)
    up_slot = 18 + jnp.where(upper, 1, 0)
    push(
        zs.at[1], zr.at[jnp.where(upper, 1, 0)], send_sem.at[20], recv_sem.at[up_slot],
        (4 * parent + place, c), climbs,
    )

    factor_end(1)
    for h in range(2):
        arrive(rt.at[h], rrecv.at[6 + h], joint)
    got(top.at[oc], 17, joint)

    @pl.when(joint)
    def _():
        wt = jnp.concatenate([rt[0], rt[1]], axis=1) - zs[1]
        sols[0] = two_pass(wt, top[...].reshape(width, width), dot_nn)
    for which in range(3):
        factor_wait(1, which)

    w3n = two_pass(w3_at[...] if False else jnp.where(has_node, w3_at[...], 0.0), factor(1, 2), dot_nn)
    got(dn.at[0], 21, climbs)

    @pl.when(has_node)
    def _():
        above = jnp.where(joint, sols[0], dn[0])
        sols[1] = w3n - two_pass(above, factor(0, 2), dot_nn)

    push(sols.at[1], dn.at[0], send_sem.at[22], recv_sem.at[21], (4 * low_child + place, c), inner)
    push(sols.at[1], dn.at[0], send_sem.at[23], recv_sem.at[21], (4 * high_child + place, c), inner)
    push(sols.at[1], dn.at[1], send_sem.at[24], recv_sem.at[22], (4 * (q + 1) + place, c), even_plane)
    w2n = two_pass(w2, factor(1, 1), dot_nn)
    w1n = two_pass(w1, factor(1, 0), dot_nn)
    got(dn.at[1], 22, odd_plane)
    above2 = jnp.where(even_plane, sols[1], dn[1])
    s1[b1] = w2n - two_pass(above2, factor(0, 1), dot_nn)
    send(s1.at[b1], s1.at[b1], 25, (yp, c))
    got(s1.at[1 - b1], 25)
    sol1 = w1n - two_pass(s1[...].reshape(quarter, width), factor(0, 0), dot_nn)
    s2[...] = sol1.reshape(2, eighth, width)
    slot = c * 2 + b0
    gath[slot] = sol1.astype(BF16)
    for t in range(1, 4):
        to_c = (c + t // 2) % 2
        to_b = (b0 + t % 2) % 2
        push(
            gath.at[slot], gath.at[slot], osend.at[t], orecv.at[t], (p - b0 + to_b, to_c),
        )

    block8 = c * 4 + b0 * 2 + b1
    for h in range(2):
        cols = pl.ds(h * half, half)
        for part_at in range(2):
            block = 2 * slot + part_at
            to = (p - b0, h)
            mine = is_even & (c == h)
            push(
                s2.at[part_at, :, cols], sep_acc.at[block], osend.at[4 + 2 * h + part_at],
                orecv.at[4 + block], to, jnp.logical_not(mine),
            )

            @pl.when(mine)
            def _():
                sep_acc[block] = s2[part_at, :, cols]

        here = (b0 == 1) & (b1 == 0) & (c == h)
        push(s1.at[b1, :, cols], sep_acc.at[block8], osend.at[8 + h], orecv.at[4 + block8], (4 * q + 1, h), jnp.logical_not(here))

        @pl.when(here)
        def _():
            sep_acc[block8] = s1[b1, :, cols]

        here = (b0 == 1) & (b1 == 1) & (c == h)
        push(sols.at[1, :, cols], sep_acc.at[block8], osend.at[10 + h], orecv.at[4 + block8], (4 * q + 3, h), has_node & jnp.logical_not(here))

        @pl.when(here & has_node)
        def _():
            sep_acc[block8] = sols[1, :, cols]

        push(sols.at[0, :, cols], sep_acc.at[block8], osend.at[12 + h], orecv.at[4 + block8], (leaves - 1, h), joint)

    for t in range(1, 4):
        from_c = (c + t // 2) % 2
        from_b = (b0 + t % 2) % 2
        arrive(gath.at[from_c * 2 + from_b], orecv.at[t])

    whole = gath[...].reshape(rows, width)
    residue = (state[...].astype(F32) - dot_nn(whole, couple[...])).astype(BF16)
    for j in range(4):
        cols = pl.ds(pl.multiple_of(oc * part + j * piece, piece), piece)
        fin_s[j] = dot_nn(residue, inv[:, cols])
        send(fin_s.at[j], fin_r.at[j], 26 + j, mate)
    for j in range(4):
        cols = pl.ds(pl.multiple_of(c * part + j * piece, piece), piece)
        value = dot_nn(residue, inv[:, cols])
        got(fin_r.at[j], 26 + j)
        leaf_out[:, pl.ds(j * piece, piece)] = value + fin_r[j]

    for block in range(8):
        bc, bb0, bb1 = block // 4, (block // 2) % 2, block % 2
        self_even = is_even & (c == bc) & (bb0 == 0)
        self_odd = (b0 == 1) & jnp.logical_not(is_top) & (c == bc) & (bb0 == 1) & (b1 == bb1)
        arrive(sep_acc.at[block], orecv.at[4 + block], jnp.logical_not(self_even | self_odd))
    sep_out[...] = sep_acc[...].reshape(rows, half)

    for cond, copy in pending:
        when(cond, lambda copy=copy: copy.wait_send())


def local(leaves, leaf_rhs, leaf_inv, leaf_couple, sep_rhs, sep_inv, sep_couple):
    _, rows, part = leaf_rhs.shape
    full = leaf_inv.shape[2]
    width = sep_inv.shape[2]
    half = width // 2
    quarter, eighth = rows // 4, rows // 8
    vmem = pl.BlockSpec(memory_space=pltpu.VMEM)
    anywhere = pl.BlockSpec(memory_space=pl.ANY)
    V = pltpu.VMEM
    dma = pltpu.SemaphoreType.DMA
    leaf_solution, sep_solution = pl.pallas_call(
        functools.partial(kernel, leaves),
        out_shape=(
            jax.ShapeDtypeStruct((rows, part), F32),
            jax.ShapeDtypeStruct((rows, half), F32),
        ),
        in_specs=[vmem, anywhere, anywhere, vmem, vmem, vmem],
        out_specs=(vmem, vmem),
        scratch_shapes=[
            V((part, full), BF16), V((width, part), BF16), V((rows, part), BF16), V((rows, part), BF16),
            V((half, width), F32), V((half, half), F32), V((2, 3, 2, half, width), BF16), V((2, half, width), BF16),
            V((2, quarter, half), F32), V((2, 2, eighth, half), F32), V((2, eighth, half), F32),
            V((2, quarter, width), F32), V((2, quarter, width), F32), V((2, quarter, width), F32),
            V((quarter, width), F32), V((quarter, width), F32), V((2, eighth, width), F32), V((eighth, width), F32),
            V((2, eighth, width), F32), V((2, eighth, width), F32), V((2, eighth, width), F32), V((2, eighth, width), F32),
            V((2, eighth, width), F32), V((2, eighth, width), F32), V((4, quarter, width), BF16),
            V((4, rows, part // 4), F32), V((4, rows, part // 4), F32), V((8, eighth, half), F32),
            dma((2,)), dma((30,)), dma((30,)), dma((20,)), dma((8,)), dma((14,)), dma((12,)),
        ],
        compiler_params=pltpu.CompilerParams(
            collective_id=0, has_side_effects=True, vmem_limit_bytes=60 * 1024 * 1024
        ),
    )(leaf_rhs[0], leaf_inv, leaf_couple, sep_rhs[0], sep_inv[0], sep_couple[0])
    return leaf_solution[None], sep_solution[None]


def solution(mesh):
    return jax.shard_map(
        functools.partial(local, mesh.shape["leaf"]),
        mesh=mesh,
        in_specs=(
            P("leaf", None, "sep"),
            P("leaf", "sep", None),
            P("leaf", None, "sep"),
            P("leaf", None, "sep"),
            P("leaf", "sep", None),
            P("leaf", None, "sep"),
        ),
        out_specs=(P("leaf", None, "sep"), P("leaf", None, "sep")),
        check_vma=False,
    )
```

```python
import functools

import jax
import jax.numpy as jnp
from jax import lax
from jax.experimental import pallas as pl
from jax.experimental.pallas import tpu as pltpu
from jax.sharding import PartitionSpec as P

F32 = jnp.float32
BF16 = jnp.bfloat16


def dot_nt(a, b):
    return lax.dot_general(a, b, (((1,), (1,)), ((), ())), preferred_element_type=F32)


def dot_nn(a, b):
    return lax.dot_general(a, b, (((1,), (0,)), ((), ())), preferred_element_type=F32)


def dot_tn(a, b):
    return lax.dot_general(a, b, (((0,), (0,)), ((), ())), preferred_element_type=F32)


def halves(value):
    high = value.astype(BF16)
    return high, (value - high.astype(F32)).astype(BF16)


def three_pass(a, b, dot):
    ah, al = halves(a)
    bh, bl = halves(b)
    return dot(ah, bh) + (dot(ah, bl) + dot(al, bh))


def two_pass(a, b, dot):
    rows = a.shape[0]
    both = dot(jnp.concatenate(halves(a), axis=0), b)
    return both[:rows] + both[rows:]


def kernel(
    leaves,
    rhs_ref, inv_hbm, couple_hbm, srhs_ref, sinv_ref, scpl_ref,
    leaf_out, sep_out,
    inv, couple, other_rhs, state, other_inv, other_cpl, fac, top,
    r1, rb, rt, part_send, part_own, part_recv, xs, xr, o1, yr,
    ys, zs, zb, zr, sols, sb, dn, s2, s1, sh, gath, fin_s, fin_r, sep_acc,
    load_sem, send_sem, recv_sem, fsend, frecv, rsend, rrecv, osend, orecv, gsend, grecv,
):
    p = lax.axis_index("leaf")
    c = lax.axis_index("sep")
    oc = 1 - c
    b0 = p % 2
    b1 = (p // 2) % 2
    q = p // 4
    planes = leaves // 4
    below_top = planes // 2 - 1
    xp = p + 1 - 2 * b0
    yp = p + 2 - 4 * b1
    rows = rhs_ref.shape[0]
    part = rhs_ref.shape[1]
    width = sinv_ref.shape[1]
    half = width // 2
    quarter = rows // 4
    eighth = rows // 8

    loads = [
        pltpu.make_async_copy(couple_hbm.at[0], couple, load_sem.at[0]),
        pltpu.make_async_copy(inv_hbm.at[0], inv, load_sem.at[1]),
    ]
    for copy in loads:
        copy.start()

    me = p * 2 + c
    count = 2 * leaves
    barrier = pltpu.get_barrier_semaphore()

    @pl.loop(1, count)
    def _(step):
        to = (me + step) % count
        pl.semaphore_signal(barrier, inc=1, device_id=(to // 2, to % 2), device_id_type=pl.DeviceIdType.MESH)

    pl.semaphore_wait(barrier, count - 1)

    pending = []

    def remote(src, dst, ssem, rsem, to):
        return pltpu.make_async_remote_copy(
            src_ref=src, dst_ref=dst, send_sem=ssem, recv_sem=rsem,
            device_id=to, device_id_type=pl.DeviceIdType.MESH,
        )

    def when(cond, action):
        if cond is None:
            action()
        else:
            @pl.when(cond)
            def _():
                action()

    def push(src, dst, ssem, rsem, to, cond=None):
        copy = remote(src, dst, ssem, rsem, to)
        when(cond, lambda: copy.start())
        pending.append((cond, copy))

    def arrive(dst, rsem, cond=None):
        copy = remote(dst, dst, send_sem.at[0], rsem, (p, oc))
        when(cond, lambda: copy.wait_recv())

    def send(src, dst, slot, to, cond=None):
        push(src, dst, send_sem.at[slot], recv_sem.at[slot], to, cond)

    def got(dst, slot, cond=None):
        arrive(dst, recv_sem.at[slot], cond)

    mate = (p, oc)
    send(sinv_ref, other_inv, 1, mate)
    send(scpl_ref.at[pl.ds(pl.multiple_of(oc * half, half), half)], other_cpl, 2, mate)
    send(rhs_ref, other_rhs, 0, mate)

    is_even = b0 == 0
    is_top = p == leaves - 1
    for t in range(4):
        tc, tb0 = t // 2, t % 2
        to = (p - b0 + tb0, tc)
        mine = (c == tc) & (b0 == tb0)
        push(
            srhs_ref.at[pl.ds(t * quarter, quarter)], r1.at[c], rsend.at[t], rrecv.at[c],
            to, is_even & jnp.logical_not(mine),
        )

        @pl.when(is_even & mine)
        def _():
            r1[c] = srhs_ref[pl.ds(t * quarter, quarter), :]

    is_odd = (b0 == 1) & jnp.logical_not(is_top)
    for t in range(8):
        tc, tb0, tb1 = t // 4, (t // 2) % 2, t % 2
        to = (4 * q + 2 * tb1 + tb0, tc)
        mine = (c == tc) & (b0 == tb0) & (b1 == tb1)
        block = srhs_ref.at[pl.ds(t * eighth, eighth)]
        push(block, rb.at[b1, c], rsend.at[4 + t], rrecv.at[2 + 2 * b1 + c], to, is_odd & jnp.logical_not(mine))

        @pl.when(is_odd & mine)
        def _():
            rb[b1, c] = srhs_ref[pl.ds(t * eighth, eighth), :]

        to = (4 * below_top + 2 * tb1 + tb0, tc)
        push(block, rt.at[c], rsend.at[12 + t], rrecv.at[6 + c], to, is_top)

    own = b0 * (1 + b1)
    got(other_inv, 1)
    got(other_cpl, 2)
    at = pl.ds(pl.multiple_of(c * half, half), half)
    ours = scpl_ref[at, :]
    m_rows = three_pass(ours, sinv_ref[...], dot_nn) + three_pass(other_cpl[...], other_inv[...], dot_nn)
    n_rows = three_pass(sinv_ref[:, at], sinv_ref[...], dot_tn) + three_pass(other_inv[:, at], other_inv[...], dot_tn)
    fac[0, own, c] = jnp.where(is_top, n_rows, m_rows).astype(BF16)
    fac[1, own, c] = n_rows.astype(BF16)
    theirs = (1 - b0) * (1 + b1)
    across = 2 - b1

    chunk = half // 4

    def share(kind, idx, path, i, to, cond=None):
        ref = fac.at[kind, idx, c, pl.ds(i * chunk, chunk)]
        push(ref, ref, fsend.at[kind, path, i], frecv.at[kind, 1 if path == 4 else path, i], to, cond)

    def shared(kind, idx, core, path, i):
        arrive(fac.at[kind, idx, core, pl.ds(i * chunk, chunk)], frecv.at[kind, path, i])

    def factor_x(kind):
        for i in range(4):
            share(kind, own, 0, i, (xp, c))
            share(kind, own, 1, i, (yp, c), b0 == 1)
        ref = fac.at[kind, own, c]
        send(ref, ref, 3 + kind, mate)

    def factor_y(kind):
        for i in range(4):
            shared(kind, theirs, c, 0, i)
            share(kind, theirs, 4, i, (yp, c), b0 == 0)
            share(kind, theirs, 2, i, mate)

    def factor_end(kind):
        for i in range(4):
            shared(kind, across, c, 1, i)
            share(kind, across, 3, i, mate)

    def factor_wait(kind, which):
        if which == 0:
            got(fac.at[kind, own, oc], 3 + kind)
        else:
            for i in range(4):
                shared(kind, (theirs, across)[which - 1], oc, 1 + which, i)

    def factor(kind, idx):
        return fac[kind, idx].reshape(width, width)

    factor_x(0)

    got(other_rhs, 0)
    loads[1].wait()
    mine_cols = pl.ds(pl.multiple_of(c * part, part), part)
    other_cols = pl.ds(pl.multiple_of(oc * part, part), part)
    piece = part // 4
    for j in range(4):
        at_j = pl.ds(j * piece, piece)
        value = dot_nt(rhs_ref[...], inv[at_j, mine_cols]) + dot_nt(other_rhs[...], inv[at_j, other_cols])
        state[:, at_j] = value.astype(BF16)
    loads[0].wait()
    mid = rows // 2
    part_send[...] = dot_nt(
        state[pl.ds(pl.multiple_of(oc * mid, mid), mid), :], couple[...]
    ).reshape(2, quarter, width)
    send(part_send, part_recv, 13, mate)
    part_own[...] = dot_nt(
        state[pl.ds(pl.multiple_of(c * mid, mid), mid), :], couple[...]
    ).reshape(2, quarter, width)
    got(part_recv, 13)
    xs[...] = (part_own[1 - b0] + part_recv[1 - b0]).astype(BF16)
    send(xs, xr, 14, (xp, c))
    factor_x(1)
    factor_y(0)
    factor_wait(0, 0)
    factor_wait(0, 1)

    for h in range(2):
        arrive(r1.at[h], rrecv.at[h], jnp.logical_not(is_even & (c == h)))
    got(xr, 14)
    taken = part_own[b0] + part_recv[b0] + xr[...].astype(F32)
    w1 = jnp.concatenate([r1[0], r1[1]], axis=1) - taken
    o1[...] = two_pass(w1, factor(0, 0), dot_nt).reshape(2, eighth, width)
    ys[...] = o1[1 - b1].astype(BF16)
    send(ys, yr, 15, (yp, c))
    factor_end(0)
    factor_wait(0, 2)
    last = q == planes - 1
    joint = q == below_top
    send(fac.at[0, 2, c], top.at[c], 16, (4 * below_top + p % 4, c), last)

    for h in range(2):
        arrive(rb.at[0, h], rrecv.at[2 + h], jnp.logical_not((b0 == 1) & (b1 == 0) & (c == h)))
    got(yr, 15)
    w2 = jnp.concatenate([rb[0, 0], rb[0, 1]], axis=1) - (o1[b1] + yr[...].astype(F32))
    out2 = two_pass(w2, factor(0, 1), dot_nt)
    even_plane = q % 2 == 0
    odd_plane = jnp.logical_not(even_plane)
    zs[0] = out2
    zb[0] = out2.astype(BF16)
    place = p % 4
    send(zb.at[0], zr.at[1], 19, (4 * (q - 1) + place, c), odd_plane)

    reach = 1
    for bit in range(leaves.bit_length()):
        reach = jnp.where((q + 1) % (2 ** (bit + 1)) == 0, 2 ** (bit + 1), reach)
    upper = (q // (2 * reach)) % 2 == 1
    parent = jnp.where(upper, q - reach, q + reach)
    has_node = jnp.logical_not(last)
    low_child = q - reach // 2
    high_child = q + reach // 2
    inner = odd_plane & has_node

    factor_y(1)
    got(top.at[c], 16, joint)
    send(top.at[c], top.at[c], 17, mate, joint)

    for h in range(2):
        arrive(rb.at[1, h], rrecv.at[4 + h], has_node & jnp.logical_not((b0 == 1) & (b1 == 1) & (c == h)))
    got(zr.at[0], 18, inner)
    got(zr.at[1], 19, has_node)
    w3_at = s2.at[0]

    @pl.when(has_node)
    def _():
        first = jnp.where(even_plane, zs[0], zr[0].astype(F32))
        w3 = jnp.concatenate([rb[1, 0], rb[1, 1]], axis=1) - (first + zr[1].astype(F32))
        w3_at[...] = w3
        out3 = two_pass(w3, factor(0, 2), dot_nt)
        zs[1] = out3
        zb[1] = out3.astype(BF16)

    climbs = has_node & jnp.logical_not(joint)
    up_slot = 18 + jnp.where(upper, 1, 0)
    push(
        zb.at[1], zr.at[jnp.where(upper, 1, 0)], send_sem.at[20], recv_sem.at[up_slot],
        (4 * parent + place, c), climbs,
    )

    factor_end(1)
    for h in range(2):
        arrive(rt.at[h], rrecv.at[6 + h], joint)
    got(top.at[oc], 17, joint)

    @pl.when(joint)
    def _():
        wt = jnp.concatenate([rt[0], rt[1]], axis=1) - zs[1]
        sols[0] = two_pass(wt, top[...].reshape(width, width), dot_nn)
    for which in range(3):
        factor_wait(1, which)

    w3n = two_pass(jnp.where(has_node, w3_at[...], 0.0), factor(1, 2), dot_nn)
    got(dn.at[0], 21, climbs)

    @pl.when(has_node)
    def _():
        above = jnp.where(joint, sols[0], dn[0].astype(F32))
        sol3 = w3n - two_pass(above, factor(0, 2), dot_nn)
        sols[1] = sol3
        sb[...] = sol3.astype(BF16)

    push(sb, dn.at[0], send_sem.at[22], recv_sem.at[21], (4 * low_child + place, c), inner)
    push(sb, dn.at[0], send_sem.at[23], recv_sem.at[21], (4 * high_child + place, c), inner)
    push(sb, dn.at[1], send_sem.at[24], recv_sem.at[22], (4 * (q + 1) + place, c), even_plane)
    w2n = two_pass(w2, factor(1, 1), dot_nn)
    w1n = two_pass(w1, factor(1, 0), dot_nn)
    got(dn.at[1], 22, odd_plane)
    above2 = jnp.where(even_plane, sb[...], dn[1])
    sol2 = w2n - dot_nn(above2, factor(0, 1))
    s1[...] = sol2
    sh[b1] = sol2.astype(BF16)
    send(sh.at[b1], sh.at[b1], 25, (yp, c))
    got(sh.at[1 - b1], 25)
    sol1 = w1n - dot_nn(sh[...].reshape(quarter, width), factor(0, 0))
    s2[...] = sol1.reshape(2, eighth, width)
    slot = c * 2 + b0
    gath[slot] = sol1.astype(BF16)
    for t in range(1, 4):
        to_c = (c + t // 2) % 2
        to_b = (b0 + t % 2) % 2
        push(
            gath.at[slot], gath.at[slot], osend.at[t], orecv.at[t], (p - b0 + to_b, to_c),
        )

    block8 = c * 4 + b0 * 2 + b1
    for h in range(2):
        cols = pl.ds(h * half, half)
        for part_at in range(2):
            block = 2 * slot + part_at
            to = (p - b0, h)
            mine = is_even & (c == h)
            push(
                s2.at[part_at, :, cols], sep_acc.at[block], osend.at[4 + 2 * h + part_at],
                orecv.at[4 + block], to, jnp.logical_not(mine),
            )

            @pl.when(mine)
            def _():
                sep_acc[block] = s2[part_at, :, cols]

        here = (b0 == 1) & (b1 == 0) & (c == h)
        push(s1.at[:, cols], sep_acc.at[block8], osend.at[8 + h], orecv.at[4 + block8], (4 * q + 1, h), jnp.logical_not(here))

        @pl.when(here)
        def _():
            sep_acc[block8] = s1[:, cols]

        here = (b0 == 1) & (b1 == 1) & (c == h)
        push(sols.at[1, :, cols], sep_acc.at[block8], osend.at[10 + h], orecv.at[4 + block8], (4 * q + 3, h), has_node & jnp.logical_not(here))

        @pl.when(here & has_node)
        def _():
            sep_acc[block8] = sols[1, :, cols]

        push(sols.at[0, :, cols], sep_acc.at[block8], osend.at[12 + h], orecv.at[4 + block8], (leaves - 1, h), joint)

    def gathered(t):
        from_c = (c + t // 2) % 2
        from_b = (b0 + t % 2) % 2
        arrive(gath.at[from_c * 2 + from_b], orecv.at[t])

    def backward(group, side):
        spans = [pl.ds(pl.multiple_of((2 * h + side) * quarter, quarter), quarter) for h in range(2)]
        whole = jnp.concatenate([gath[side], gath[2 + side]], axis=0)
        before = jnp.concatenate([state[spans[0], :], state[spans[1], :]], axis=0).astype(F32)
        residue = (before - dot_nn(whole, couple[...])).astype(BF16)
        for j in range(4):
            cols = pl.ds(pl.multiple_of(oc * part + j * piece, piece), piece)
            fin_s[group, j] = dot_nn(residue, inv[:, cols]).astype(BF16)
            push(fin_s.at[group, j], fin_r.at[group, j], gsend.at[group, j], grecv.at[group, j], mate)
        for j in range(4):
            cols = pl.ds(pl.multiple_of(c * part + j * piece, piece), piece)
            value = dot_nn(residue, inv[:, cols])
            for h in range(2):
                leaf_out[spans[h], pl.ds(j * piece, piece)] = value[h * quarter:(h + 1) * quarter]
        return spans

    gathered(2)
    spans = [backward(0, b0)]
    gathered(1)
    gathered(3)
    spans.append(backward(1, 1 - b0))
    for group in range(2):
        for j in range(4):
            arrive(fin_r.at[group, j], grecv.at[group, j])
            for h in range(2):
                leaf_out[spans[group][h], pl.ds(j * piece, piece)] += fin_r[group, j, pl.ds(h * quarter, quarter)].astype(F32)

    for block in range(8):
        bc, bb0, bb1 = block // 4, (block // 2) % 2, block % 2
        self_even = is_even & (c == bc) & (bb0 == 0)
        self_odd = (b0 == 1) & jnp.logical_not(is_top) & (c == bc) & (bb0 == 1) & (b1 == bb1)
        arrive(sep_acc.at[block], orecv.at[4 + block], jnp.logical_not(self_even | self_odd))
    sep_out[...] = sep_acc[...].reshape(rows, half)

    for cond, copy in pending:
        when(cond, lambda copy=copy: copy.wait_send())


def local(leaves, leaf_rhs, leaf_inv, leaf_couple, sep_rhs, sep_inv, sep_couple):
    _, rows, part = leaf_rhs.shape
    full = leaf_inv.shape[2]
    width = sep_inv.shape[2]
    half = width // 2
    quarter, eighth = rows // 4, rows // 8
    vmem = pl.BlockSpec(memory_space=pltpu.VMEM)
    anywhere = pl.BlockSpec(memory_space=pl.ANY)
    V = pltpu.VMEM
    dma = pltpu.SemaphoreType.DMA
    leaf_solution, sep_solution = pl.pallas_call(
        functools.partial(kernel, leaves),
        out_shape=(pltpu.VMEM((rows, part), F32), pltpu.VMEM((rows, half), F32)),
        in_specs=[vmem, anywhere, anywhere, vmem, vmem, vmem],
        out_specs=(vmem, vmem),
        scratch_shapes=[
            V((part, full), BF16), V((width, part), BF16), V((rows, part), BF16), V((rows, part), BF16),
            V((half, width), F32), V((half, half), F32), V((2, 3, 2, half, width), BF16), V((2, half, width), BF16),
            V((2, quarter, half), F32), V((2, 2, eighth, half), F32), V((2, eighth, half), F32),
            V((2, quarter, width), F32), V((2, quarter, width), F32), V((2, quarter, width), F32),
            V((quarter, width), BF16), V((quarter, width), BF16), V((2, eighth, width), F32), V((eighth, width), BF16),
            V((eighth, width), BF16), V((2, eighth, width), F32), V((2, eighth, width), BF16), V((2, eighth, width), BF16),
            V((2, eighth, width), F32), V((eighth, width), BF16), V((2, eighth, width), BF16), V((2, eighth, width), F32),
            V((eighth, width), F32), V((2, eighth, width), BF16), V((4, quarter, width), BF16),
            V((2, 4, rows // 2, part // 4), BF16), V((2, 4, rows // 2, part // 4), BF16), V((8, eighth, half), F32),
            dma((2,)), dma((30,)), dma((30,)), dma((2, 5, 4)), dma((2, 5, 4)), dma((20,)), dma((8,)), dma((14,)), dma((12,)),
            dma((2, 4)), dma((2, 4)),
        ],
        compiler_params=pltpu.CompilerParams(
            collective_id=0, has_side_effects=True, vmem_limit_bytes=60 * 1024 * 1024
        ),
    )(leaf_rhs[0], leaf_inv, leaf_couple, sep_rhs[0], sep_inv[0], sep_couple[0])
    return leaf_solution[None], sep_solution[None]


def solution(mesh):
    return jax.shard_map(
        functools.partial(local, mesh.shape["leaf"]),
        mesh=mesh,
        in_specs=(
            P("leaf", None, "sep"),
            P("leaf", "sep", None),
            P("leaf", None, "sep"),
            P("leaf", None, "sep"),
            P("leaf", "sep", None),
            P("leaf", None, "sep"),
        ),
        out_specs=(P("leaf", None, "sep"), P("leaf", None, "sep")),
        check_vma=False,
    )
```

```python
import functools

import jax
import jax.numpy as jnp
from jax import lax
from jax.experimental import pallas as pl
from jax.experimental.pallas import tpu as pltpu
from jax.sharding import PartitionSpec as P

F32 = jnp.float32
BF16 = jnp.bfloat16


def dot_nt(a, b):
    return lax.dot_general(a, b, (((1,), (1,)), ((), ())), preferred_element_type=F32)


def dot_nn(a, b):
    return lax.dot_general(a, b, (((1,), (0,)), ((), ())), preferred_element_type=F32)


def dot_tn(a, b):
    return lax.dot_general(a, b, (((0,), (0,)), ((), ())), preferred_element_type=F32)


def halves(value):
    high = value.astype(BF16)
    return high, (value - high.astype(F32)).astype(BF16)


def three_pass(a, b, dot):
    ah, al = halves(a)
    bh, bl = halves(b)
    return dot(ah, bh) + (dot(ah, bl) + dot(al, bh))


def two_pass(a, b, dot):
    rows = a.shape[0]
    both = dot(jnp.concatenate(halves(a), axis=0), b)
    return both[:rows] + both[rows:]


def kernel(
    leaves,
    rhs_ref, inv_hbm, couple_hbm, srhs_ref, sinv_ref, scpl_ref,
    leaf_out, sep_out,
    inv, couple, other_rhs, state, other_inv, other_cpl, fac, top,
    r1, rb, rt, part_send, part_own, part_recv, xs, xr, o1, yr,
    ys, zs, zb, zr, sols, sb, dn, s2, s1, sh, gath, fin_s, fin_r, sep_acc,
    load_sem, send_sem, recv_sem, fsend, frecv, rsend, rrecv, osend, orecv, gsend, grecv, tsend, trecv,
):
    p = lax.axis_index("leaf")
    c = lax.axis_index("sep")
    oc = 1 - c
    b0 = p % 2
    b1 = (p // 2) % 2
    q = p // 4
    planes = leaves // 4
    below_top = planes // 2 - 1
    xp = p + 1 - 2 * b0
    yp = p + 2 - 4 * b1
    rows = rhs_ref.shape[0]
    part = rhs_ref.shape[1]
    width = sinv_ref.shape[1]
    half = width // 2
    quarter = rows // 4
    eighth = rows // 8

    loads = [
        pltpu.make_async_copy(couple_hbm.at[0], couple, load_sem.at[0]),
        pltpu.make_async_copy(inv_hbm.at[0], inv, load_sem.at[1]),
    ]
    for copy in loads:
        copy.start()

    me = p * 2 + c
    count = 2 * leaves
    barrier = pltpu.get_barrier_semaphore()

    @pl.loop(1, count)
    def _(step):
        to = (me + step) % count
        pl.semaphore_signal(barrier, inc=1, device_id=(to // 2, to % 2), device_id_type=pl.DeviceIdType.MESH)

    pl.semaphore_wait(barrier, count - 1)

    pending = []

    def remote(src, dst, ssem, rsem, to):
        return pltpu.make_async_remote_copy(
            src_ref=src, dst_ref=dst, send_sem=ssem, recv_sem=rsem,
            device_id=to, device_id_type=pl.DeviceIdType.MESH,
        )

    def when(cond, action):
        if cond is None:
            action()
        else:
            @pl.when(cond)
            def _():
                action()

    def push(src, dst, ssem, rsem, to, cond=None):
        copy = remote(src, dst, ssem, rsem, to)
        when(cond, lambda: copy.start())
        pending.append((cond, copy))

    def arrive(dst, rsem, cond=None):
        copy = remote(dst, dst, send_sem.at[0], rsem, (p, oc))
        when(cond, lambda: copy.wait_recv())

    def send(src, dst, slot, to, cond=None):
        push(src, dst, send_sem.at[slot], recv_sem.at[slot], to, cond)

    def got(dst, slot, cond=None):
        arrive(dst, recv_sem.at[slot], cond)

    mate = (p, oc)
    send(sinv_ref, other_inv, 1, mate)
    send(scpl_ref.at[pl.ds(pl.multiple_of(oc * half, half), half)], other_cpl, 2, mate)
    send(rhs_ref, other_rhs, 0, mate)

    is_even = b0 == 0
    is_top = p == leaves - 1
    for t in range(4):
        tc, tb0 = t // 2, t % 2
        to = (p - b0 + tb0, tc)
        mine = (c == tc) & (b0 == tb0)
        push(
            srhs_ref.at[pl.ds(t * quarter, quarter)], r1.at[c], rsend.at[t], rrecv.at[c],
            to, is_even & jnp.logical_not(mine),
        )

        @pl.when(is_even & mine)
        def _():
            r1[c] = srhs_ref[pl.ds(t * quarter, quarter), :]

    is_odd = (b0 == 1) & jnp.logical_not(is_top)
    for t in range(8):
        tc, tb0, tb1 = t // 4, (t // 2) % 2, t % 2
        to = (4 * q + 2 * tb1 + tb0, tc)
        mine = (c == tc) & (b0 == tb0) & (b1 == tb1)
        block = srhs_ref.at[pl.ds(t * eighth, eighth)]
        push(block, rb.at[b1, c], rsend.at[4 + t], rrecv.at[2 + 2 * b1 + c], to, is_odd & jnp.logical_not(mine))

        @pl.when(is_odd & mine)
        def _():
            rb[b1, c] = srhs_ref[pl.ds(t * eighth, eighth), :]

        to = (4 * below_top + 2 * tb1 + tb0, tc)
        push(block, rt.at[c], rsend.at[12 + t], rrecv.at[6 + c], to, is_top)

    own = b0 * (1 + b1)
    got(other_inv, 1)
    got(other_cpl, 2)
    at = pl.ds(pl.multiple_of(c * half, half), half)
    ours = scpl_ref[at, :]

    def n_rows():
        mine, other = sinv_ref[:, at], other_inv[:, at]
        return (three_pass(mine, sinv_ref[...], dot_tn) + three_pass(other, other_inv[...], dot_tn)).astype(BF16)

    @pl.when(is_top)
    def _():
        fac[0, own, c] = n_rows()

    @pl.when(jnp.logical_not(is_top))
    def _():
        m_rows = three_pass(ours, sinv_ref[...], dot_nn) + three_pass(other_cpl[...], other_inv[...], dot_nn)
        fac[0, own, c] = m_rows.astype(BF16)

    theirs = (1 - b0) * (1 + b1)
    across = 2 - b1

    chunk = half // 4
    last = q == planes - 1
    joint = q == below_top
    place = p % 4

    def top_share(i, cond):
        span = pl.ds(i * chunk, chunk)
        push(
            fac.at[0, 2, c, span], top.at[c, span], tsend.at[i], trecv.at[i],
            (4 * below_top + place, c), last & cond,
        )

    def share(kind, idx, path, i, to, cond=None):
        ref = fac.at[kind, idx, c, pl.ds(i * chunk, chunk)]
        push(ref, ref, fsend.at[kind, path, i], frecv.at[kind, 1 if path == 4 else path, i], to, cond)

    def shared(kind, idx, core, path, i, cond=None):
        arrive(fac.at[kind, idx, core, pl.ds(i * chunk, chunk)], frecv.at[kind, path, i], cond)

    def factor_x(kind):
        for i in range(4):
            share(kind, own, 0, i, (xp, c))
            if kind == 0:
                share(kind, own, 1, i, (yp, c), b0 == 1)
                top_share(i, (b0 == 1) & (b1 == 1))
        ref = fac.at[kind, own, c]
        send(ref, ref, 3 + kind, mate)

    def factor_y(kind):
        for i in range(4):
            shared(kind, theirs, c, 0, i)
            share(kind, theirs, 4, i, (yp, c), b0 == 0)
            share(kind, theirs, 2, i, mate)
            if kind == 0:
                top_share(i, (b0 == 0) & (b1 == 1))

    def factor_end(kind, cond=None):
        for i in range(4):
            shared(kind, across, c, 1, i, cond)
            share(kind, across, 3, i, mate, cond)

    def factor_wait(kind, which):
        if which == 0:
            got(fac.at[kind, own, oc], 3 + kind)
        else:
            for i in range(4):
                shared(kind, (theirs, across)[which - 1], oc, 1 + which, i)

    def factor(kind, idx):
        return fac[kind, idx].reshape(width, width)

    factor_x(0)
    fac[1, own, c] = n_rows()

    got(other_rhs, 0)
    loads[1].wait()
    mine_cols = pl.ds(pl.multiple_of(c * part, part), part)
    other_cols = pl.ds(pl.multiple_of(oc * part, part), part)
    piece = part // 4
    for j in range(4):
        at_j = pl.ds(j * piece, piece)
        value = dot_nt(rhs_ref[...], inv[at_j, mine_cols]) + dot_nt(other_rhs[...], inv[at_j, other_cols])
        state[:, at_j] = value.astype(BF16)
    loads[0].wait()
    mid = rows // 2
    part_send[...] = dot_nt(
        state[pl.ds(pl.multiple_of(oc * mid, mid), mid), :], couple[...]
    ).reshape(2, quarter, width)
    send(part_send, part_recv, 13, mate)
    part_own[...] = dot_nt(
        state[pl.ds(pl.multiple_of(c * mid, mid), mid), :], couple[...]
    ).reshape(2, quarter, width)
    got(part_recv, 13)
    xs[...] = (part_own[1 - b0] + part_recv[1 - b0]).astype(BF16)
    send(xs, xr, 14, (xp, c))
    factor_x(1)
    factor_y(0)
    factor_end(0, b0 == 1)
    for i in range(4):
        top_share(i, (b0 == 1) & (b1 == 0))
    factor_wait(0, 0)
    factor_wait(0, 1)

    for h in range(2):
        arrive(r1.at[h], rrecv.at[h], jnp.logical_not(is_even & (c == h)))
    got(xr, 14)
    taken = part_own[b0] + part_recv[b0] + xr[...].astype(F32)
    w1 = jnp.concatenate([r1[0], r1[1]], axis=1) - taken
    o1[...] = two_pass(w1, factor(0, 0), dot_nt).reshape(2, eighth, width)
    ys[...] = o1[1 - b1].astype(BF16)
    send(ys, yr, 15, (yp, c))
    for i in range(4):
        share(1, own, 1, i, (yp, c), b0 == 1)
    factor_end(0, b0 == 0)
    factor_wait(0, 2)

    for h in range(2):
        arrive(rb.at[0, h], rrecv.at[2 + h], jnp.logical_not((b0 == 1) & (b1 == 0) & (c == h)))
    got(yr, 15)
    w2 = jnp.concatenate([rb[0, 0], rb[0, 1]], axis=1) - (o1[b1] + yr[...].astype(F32))
    out2 = two_pass(w2, factor(0, 1), dot_nt)
    even_plane = q % 2 == 0
    odd_plane = jnp.logical_not(even_plane)
    zs[0] = out2
    zb[0] = out2.astype(BF16)
    send(zb.at[0], zr.at[1], 19, (4 * (q - 1) + place, c), odd_plane)
    for i in range(4):
        top_share(i, (b0 == 0) & (b1 == 0))

    reach = 1
    for bit in range(leaves.bit_length()):
        reach = jnp.where((q + 1) % (2 ** (bit + 1)) == 0, 2 ** (bit + 1), reach)
    upper = (q // (2 * reach)) % 2 == 1
    parent = jnp.where(upper, q - reach, q + reach)
    has_node = jnp.logical_not(last)
    low_child = q - reach // 2
    high_child = q + reach // 2
    inner = odd_plane & has_node

    factor_y(1)
    for i in range(4):
        arrive(top.at[c, pl.ds(i * chunk, chunk)], trecv.at[i], joint)
    send(top.at[c], top.at[c], 17, mate, joint)

    for h in range(2):
        arrive(rb.at[1, h], rrecv.at[4 + h], has_node & jnp.logical_not((b0 == 1) & (b1 == 1) & (c == h)))
    got(zr.at[0], 18, inner)
    got(zr.at[1], 19, has_node)
    w3_at = s2.at[0]

    @pl.when(has_node)
    def _():
        first = jnp.where(even_plane, zs[0], zr[0].astype(F32))
        w3 = jnp.concatenate([rb[1, 0], rb[1, 1]], axis=1) - (first + zr[1].astype(F32))
        w3_at[...] = w3
        out3 = two_pass(w3, factor(0, 2), dot_nt)
        zs[1] = out3
        zb[1] = out3.astype(BF16)

    climbs = has_node & jnp.logical_not(joint)
    up_slot = 18 + jnp.where(upper, 1, 0)
    push(
        zb.at[1], zr.at[jnp.where(upper, 1, 0)], send_sem.at[20], recv_sem.at[up_slot],
        (4 * parent + place, c), climbs,
    )

    factor_end(1)
    for h in range(2):
        arrive(rt.at[h], rrecv.at[6 + h], joint)
    got(top.at[oc], 17, joint)

    @pl.when(joint)
    def _():
        wt = jnp.concatenate([rt[0], rt[1]], axis=1) - zs[1]
        sols[0] = two_pass(wt, top[...].reshape(width, width), dot_nn)
    for which in range(3):
        factor_wait(1, which)

    w3n = two_pass(jnp.where(has_node, w3_at[...], 0.0), factor(1, 2), dot_nn)
    got(dn.at[0], 21, climbs)

    @pl.when(has_node)
    def _():
        above = jnp.where(joint, sols[0], dn[0].astype(F32))
        sol3 = w3n - two_pass(above, factor(0, 2), dot_nn)
        sols[1] = sol3
        sb[...] = sol3.astype(BF16)

    push(sb, dn.at[0], send_sem.at[22], recv_sem.at[21], (4 * low_child + place, c), inner)
    push(sb, dn.at[0], send_sem.at[23], recv_sem.at[21], (4 * high_child + place, c), inner)
    push(sb, dn.at[1], send_sem.at[24], recv_sem.at[22], (4 * (q + 1) + place, c), even_plane)
    w2n = two_pass(w2, factor(1, 1), dot_nn)
    w1n = two_pass(w1, factor(1, 0), dot_nn)
    got(dn.at[1], 22, odd_plane)
    above2 = jnp.where(even_plane, sb[...], dn[1])
    sol2 = w2n - dot_nn(above2, factor(0, 1))
    s1[...] = sol2
    sh[b1] = sol2.astype(BF16)
    send(sh.at[b1], sh.at[b1], 25, (yp, c))
    got(sh.at[1 - b1], 25)
    sol1 = w1n - dot_nn(sh[...].reshape(quarter, width), factor(0, 0))
    s2[...] = sol1.reshape(2, eighth, width)
    slot = c * 2 + b0
    gath[slot] = sol1.astype(BF16)
    for t in range(1, 4):
        to_c = (c + t // 2) % 2
        to_b = (b0 + t % 2) % 2
        push(
            gath.at[slot], gath.at[slot], osend.at[t], orecv.at[t], (p - b0 + to_b, to_c),
        )

    block8 = c * 4 + b0 * 2 + b1
    for h in range(2):
        cols = pl.ds(h * half, half)
        for part_at in range(2):
            block = 2 * slot + part_at
            to = (p - b0, h)
            mine = is_even & (c == h)
            push(
                s2.at[part_at, :, cols], sep_acc.at[block], osend.at[4 + 2 * h + part_at],
                orecv.at[4 + block], to, jnp.logical_not(mine),
            )

            @pl.when(mine)
            def _():
                sep_acc[block] = s2[part_at, :, cols]

        here = (b0 == 1) & (b1 == 0) & (c == h)
        push(s1.at[:, cols], sep_acc.at[block8], osend.at[8 + h], orecv.at[4 + block8], (4 * q + 1, h), jnp.logical_not(here))

        @pl.when(here)
        def _():
            sep_acc[block8] = s1[:, cols]

        here = (b0 == 1) & (b1 == 1) & (c == h)
        push(sols.at[1, :, cols], sep_acc.at[block8], osend.at[10 + h], orecv.at[4 + block8], (4 * q + 3, h), has_node & jnp.logical_not(here))

        @pl.when(here & has_node)
        def _():
            sep_acc[block8] = sols[1, :, cols]

        push(sols.at[0, :, cols], sep_acc.at[block8], osend.at[12 + h], orecv.at[4 + block8], (leaves - 1, h), joint)

    def gathered(t):
        from_c = (c + t // 2) % 2
        from_b = (b0 + t % 2) % 2
        arrive(gath.at[from_c * 2 + from_b], orecv.at[t])

    def backward(group, side):
        spans = [pl.ds(pl.multiple_of((2 * h + side) * quarter, quarter), quarter) for h in range(2)]
        whole = jnp.concatenate([gath[side], gath[2 + side]], axis=0)
        before = jnp.concatenate([state[spans[0], :], state[spans[1], :]], axis=0).astype(F32)
        residue = (before - dot_nn(whole, couple[...])).astype(BF16)
        for j in range(4):
            cols = pl.ds(pl.multiple_of(oc * part + j * piece, piece), piece)
            fin_s[group, j] = dot_nn(residue, inv[:, cols]).astype(BF16)
            push(fin_s.at[group, j], fin_r.at[group, j], gsend.at[group, j], grecv.at[group, j], mate)
        for j in range(4):
            cols = pl.ds(pl.multiple_of(c * part + j * piece, piece), piece)
            value = dot_nn(residue, inv[:, cols])
            for h in range(2):
                leaf_out[spans[h], pl.ds(j * piece, piece)] = value[h * quarter:(h + 1) * quarter]
        return spans

    gathered(2)
    spans = [backward(0, b0)]
    gathered(1)
    gathered(3)
    spans.append(backward(1, 1 - b0))
    for group in range(2):
        for j in range(4):
            arrive(fin_r.at[group, j], grecv.at[group, j])
            for h in range(2):
                leaf_out[spans[group][h], pl.ds(j * piece, piece)] += fin_r[group, j, pl.ds(h * quarter, quarter)].astype(F32)

    for block in range(8):
        bc, bb0, bb1 = block // 4, (block // 2) % 2, block % 2
        self_even = is_even & (c == bc) & (bb0 == 0)
        self_odd = (b0 == 1) & jnp.logical_not(is_top) & (c == bc) & (bb0 == 1) & (b1 == bb1)
        arrive(sep_acc.at[block], orecv.at[4 + block], jnp.logical_not(self_even | self_odd))
    sep_out[...] = sep_acc[...].reshape(rows, half)

    for cond, copy in pending:
        when(cond, lambda copy=copy: copy.wait_send())


def local(leaves, leaf_rhs, leaf_inv, leaf_couple, sep_rhs, sep_inv, sep_couple):
    _, rows, part = leaf_rhs.shape
    full = leaf_inv.shape[2]
    width = sep_inv.shape[2]
    half = width // 2
    quarter, eighth = rows // 4, rows // 8
    vmem = pl.BlockSpec(memory_space=pltpu.VMEM)
    anywhere = pl.BlockSpec(memory_space=pl.ANY)
    V = pltpu.VMEM
    dma = pltpu.SemaphoreType.DMA
    leaf_solution, sep_solution = pl.pallas_call(
        functools.partial(kernel, leaves),
        out_shape=(pltpu.VMEM((rows, part), F32), pltpu.VMEM((rows, half), F32)),
        in_specs=[vmem, anywhere, anywhere, vmem, vmem, vmem],
        out_specs=(vmem, vmem),
        scratch_shapes=[
            V((part, full), BF16), V((width, part), BF16), V((rows, part), BF16), V((rows, part), BF16),
            V((half, width), F32), V((half, half), F32), V((2, 3, 2, half, width), BF16), V((2, half, width), BF16),
            V((2, quarter, half), F32), V((2, 2, eighth, half), F32), V((2, eighth, half), F32),
            V((2, quarter, width), F32), V((2, quarter, width), F32), V((2, quarter, width), F32),
            V((quarter, width), BF16), V((quarter, width), BF16), V((2, eighth, width), F32), V((eighth, width), BF16),
            V((eighth, width), BF16), V((2, eighth, width), F32), V((2, eighth, width), BF16), V((2, eighth, width), BF16),
            V((2, eighth, width), F32), V((eighth, width), BF16), V((2, eighth, width), BF16), V((2, eighth, width), F32),
            V((eighth, width), F32), V((2, eighth, width), BF16), V((4, quarter, width), BF16),
            V((2, 4, rows // 2, part // 4), BF16), V((2, 4, rows // 2, part // 4), BF16), V((8, eighth, half), F32),
            dma((2,)), dma((30,)), dma((30,)), dma((2, 5, 4)), dma((2, 5, 4)), dma((20,)), dma((8,)), dma((14,)), dma((12,)),
            dma((2, 4)), dma((2, 4)), dma((4,)), dma((4,)),
        ],
        compiler_params=pltpu.CompilerParams(
            collective_id=0, has_side_effects=True, vmem_limit_bytes=60 * 1024 * 1024
        ),
    )(leaf_rhs[0], leaf_inv, leaf_couple, sep_rhs[0], sep_inv[0], sep_couple[0])
    return leaf_solution[None], sep_solution[None]


def solution(mesh):
    return jax.shard_map(
        functools.partial(local, mesh.shape["leaf"]),
        mesh=mesh,
        in_specs=(
            P("leaf", None, "sep"),
            P("leaf", "sep", None),
            P("leaf", None, "sep"),
            P("leaf", None, "sep"),
            P("leaf", "sep", None),
            P("leaf", None, "sep"),
        ),
        out_specs=(P("leaf", None, "sep"), P("leaf", None, "sep")),
        check_vma=False,
    )
```
